32 devices in a mesh: rep: 8 (over z, core), shard: 4 (over y, x).
Axes of the slice: x: 2, y: 2, z: 4, core: 2. Of those that a mesh axis runs over, the one named last changes fastest.
Arguments:
- tokens: bfloat16 [8192, 1600], P(('rep', 'shard')), may hold values from -6 to 6
- attn_gain: bfloat16 [1600], P('shard'), may hold values from 0.099609375 to 1.8984375
- attn_shift: bfloat16 [1600], P('shard'), may hold values from -3 to 3
- qkv_weight: bfloat16 [1600, 4800], P('shard'), may hold values from -1 to 1, as said below
- qv_bias: bfloat16 [3200], P('shard'), may hold values from -1.25 to 1.25
- out_weight: bfloat16 [1600, 1600], P('shard'), may hold values from -0.625 to 0.625
- out_bias: bfloat16 [1600], P('shard'), may hold values from -3 to 3
- mlp_gain: bfloat16 [1600], P('shard'), may hold values from 0.099609375 to 1.8984375
- mlp_shift: bfloat16 [1600], P('shard'), may hold values from -3 to 3
- fc_weight: bfloat16 [1600, 6400], P('shard'), may hold values from -0.15625 to 0.15625
- fc_bias: bfloat16 [6400], P('shard'), may hold values from -3 to 3
- proj_weight: bfloat16 [6400, 1600], P('shard'), may hold values from -0.078125 to 0.078125
- proj_bias: bfloat16 [1600], P('shard'), may hold values from -3 to 3
- out_grad: bfloat16 [8192, 1600], P(('rep', 'shard')), may hold values from -6 to 6
- segment_ids: int32 [8192], P(('rep', 'shard')), may hold values from 0 to 256, as said below
Outputs:
- block_out: bfloat16 [8192, 1600], P(('rep', 'shard'))
- tokens_grad: bfloat16 [8192, 1600], P(('rep', 'shard'))
- attn_gain_grad: float32 [1600], P('shard')
- attn_shift_grad: float32 [1600], P('shard')
- qkv_weight_grad: float32 [1600, 4800], P('shard')
- qv_bias_grad: float32 [3200], P('shard')
- out_weight_grad: float32 [1600, 1600], P('shard')
- out_bias_grad: float32 [1600], P('shard')
- mlp_gain_grad: float32 [1600], P('shard')
- mlp_shift_grad: float32 [1600], P('shard')
- fc_weight_grad: float32 [1600, 6400], P('shard')
- fc_bias_grad: float32 [6400], P('shard')
- proj_weight_grad: float32 [6400, 1600], P('shard')
- proj_bias_grad: float32 [1600], P('shard')
The draws below stay inside these ranges and needn't reach their ends.
Inputs may be any that keep to these rules, and one draw needn't show every extreme that they name: `segment_ids`: within each device's block of 256 slots the live tokens come first, numbered 0 for the first sequence and 1 for the second, never falling; slots past the device's token count hold 256; every device holds 128 tokens or more, some device holds exactly 128 and some is full. `qkv_weight`: columns are the queries, the keys and the values, in that order.
All inputs are finite; a program needn't handle non-finite values.
Results may differ from the reference program's by a relative error of at most 0.019.
Values may be sent and summed in bfloat16 or wider, within the bound.
A program may use at most 320 MiB of HBM per device.

```python
import jax
import jax.numpy as jnp
from jax import lax

D = 1600
H = 25
HD = 64
FF = 6400
CAP = 256
MIN_TOK = 128
TOKENS = 8192


def draw_segment_ids(key, part):
    blocks = TOKENS // CAP
    first_key, second_key = jax.random.split(key)
    device = jnp.arange(blocks, dtype=jnp.int32)
    drawn = jax.random.randint(first_key, (blocks,), MIN_TOK, CAP + 1, dtype=jnp.int32)
    counts = jnp.where(device % 4 == 0, CAP, jnp.where(device % 4 == 1, MIN_TOK, drawn))
    spread = jax.random.randint(second_key, (blocks,), 0, 1000, dtype=jnp.int32)
    lowest = counts // 3
    border = lowest + spread * (counts - lowest) // 1000
    position = jnp.arange(CAP, dtype=jnp.int32)[None, :]
    labels = jnp.where(position < border[:, None], 0, jnp.where(position < counts[:, None], 1, CAP))
    return labels.reshape(TOKENS).astype(jnp.int32)


def draw_qkv_weight(key, part):
    base = jax.random.truncated_normal(key, -4.0, 4.0, (D, 3 * D), jnp.float32)
    base = base * D ** (-0.5)
    return base.astype(jnp.bfloat16)


def levels(own_key, extent, shards, low, high):
    loudness = 1.0
    for axis_at, shards_of in shards:
        steps = jax.random.uniform(jax.random.fold_in(jax.random.fold_in(own_key, 6), axis_at), (shards_of,), jnp.float32, low / len(shards), high / len(shards))
        loudness = loudness * jnp.repeat(jnp.exp(steps), extent[axis_at] // shards_of).reshape((-1,) + (1,) * (len(extent) - 1 - axis_at))
    return loudness


def scatter_about(stream_key, shape, width, limit, shards=(), kind=jnp.bfloat16):
    values = jax.random.normal(stream_key, shape, jnp.float32) * width
    if len(shards) > 0:
        values = levels(stream_key, shape, shards, -0.22, 0.18) * values
    return jnp.clip(values, min=-limit, max=limit).astype(kind)


def setup_inputs(seed: int = 0) -> dict:
    keys = jax.random.split(jax.random.key(seed), 16)
    tokens = scatter_about(keys[0], (TOKENS, D), 1.0, 6.0, ((0, 32),))
    attn_gain = jnp.clip(1.0 + 0.18 * jax.random.normal(keys[1], (D,), jnp.float32), 0.099609375, 1.8984375).astype(jnp.bfloat16)
    attn_shift = scatter_about(keys[2], (D,), 0.5, 3.0, ((0, 4),))
    qkv_weight = draw_qkv_weight(jax.random.fold_in(keys[15], 71), 0)
    qv_bias = scatter_about(keys[4], (2 * D,), 0.2, 1.25, ((0, 4),))
    out_weight = scatter_about(keys[5], (D, D), (D // 16) ** -0.5, 0.625, ((0, 4),))
    out_bias = scatter_about(keys[6], (D,), 0.5, 3.0, ((0, 4),))
    mlp_gain = jnp.clip(1.0 + 0.18 * jax.random.normal(keys[7], (D,), jnp.float32), 0.099609375, 1.8984375).astype(jnp.bfloat16)
    mlp_shift = scatter_about(keys[8], (D,), 0.5, 3.0, ((0, 4),))
    fc_weight = scatter_about(keys[9], (D, FF), D ** -0.5, 0.15625, ((0, 4),))
    fc_bias = scatter_about(keys[10], (FF,), 0.5, 3.0, ((0, 4),))
    proj_weight = scatter_about(keys[11], (FF, D), FF ** -0.5, 0.078125, ((0, 4),))
    proj_bias = scatter_about(keys[12], (D,), 0.5, 3.0, ((0, 4),))
    out_grad = scatter_about(keys[13], (TOKENS, D), 1.0, 6.0, ((0, 32),))
    segment_ids = draw_segment_ids(jax.random.fold_in(keys[15], 71), 0)
    return {"tokens": tokens, "attn_gain": attn_gain, "attn_shift": attn_shift, "qkv_weight": qkv_weight, "qv_bias": qv_bias, "out_weight": out_weight, "out_bias": out_bias, "mlp_gain": mlp_gain, "mlp_shift": mlp_shift, "fc_weight": fc_weight, "fc_bias": fc_bias, "proj_weight": proj_weight, "proj_bias": proj_bias, "out_grad": out_grad, "segment_ids": segment_ids}


@jax.custom_vjp
def low(v):
    return lax.optimization_barrier(v.astype(jnp.bfloat16)).astype(jnp.float32)

@jax.custom_vjp
def low_back(v):
    return v

def low_keep(v):
    return (low(v), None)

def low_pass(kept, grad):
    return (grad,)

def back_keep(v):
    return (v, None)

def back_low(kept, grad):
    return (low(grad),)
low.defvjp(low_keep, low_pass)
low_back.defvjp(back_keep, back_low)

def matmul(left, right):
    return jnp.dot(left, right, precision=lax.Precision.HIGHEST, preferred_element_type=jnp.float32)

def layer_norm(values, gain, shift):
    centre = values - lax.optimization_barrier(jnp.mean(values, axis=-1, keepdims=True))
    spread = lax.optimization_barrier(jnp.mean(centre * centre, axis=-1, keepdims=True))
    return centre * lax.rsqrt(spread + 1e-05) * gain + shift

def gelu_tanh(values):
    return jax.nn.gelu(values, approximate=True)

def attend_block(pieces):
    queries, key_vecs, value_vecs, block_ids = pieces
    positions = jnp.arange(CAP)
    allowed = (block_ids[:, None] == block_ids[None, :]) & (positions[None, :] <= positions[:, None])
    scores = jnp.einsum('qhd,khd->hqk', queries, key_vecs, precision=lax.Precision.HIGHEST) * HD ** (-0.5)
    scores = jnp.where(allowed[None], low_back(scores), -1e+30)
    logsum = jax.nn.logsumexp(scores, axis=-1, keepdims=True)
    prob_low = low(jnp.exp(scores - logsum))
    return jnp.einsum('hqk,khd->qhd', prob_low, value_vecs, precision=lax.Precision.HIGHEST)

def forward(inputs, attn_gain, attn_shift, qkv_weight, qv_bias, out_weight, out_bias, mlp_gain, mlp_shift, fc_weight, fc_bias, proj_weight, proj_bias, live_rows, segment_ids):
    blocks = TOKENS // CAP
    norm_one = low(layer_norm(inputs, attn_gain, attn_shift))
    projected = matmul(norm_one, qkv_weight)
    queries = low(low_back(projected[:, 0:D] + qv_bias[0:D]))
    key_vecs = low(low_back(projected[:, D:2 * D]))
    value_vecs = low(low_back(projected[:, 2 * D:3 * D] + qv_bias[D:2 * D]))
    block_shape = (blocks, CAP, H, HD)
    mixed_heads = lax.map(jax.checkpoint(attend_block), (queries.reshape(block_shape), key_vecs.reshape(block_shape), value_vecs.reshape(block_shape), segment_ids.reshape(blocks, CAP)))
    mixed_heads = low(low_back(mixed_heads.reshape(TOKENS, D)))
    residual = inputs + low_back(matmul(mixed_heads, out_weight) + out_bias)
    norm_two = low(layer_norm(residual, mlp_gain, mlp_shift))
    hidden = low(gelu_tanh(low_back(matmul(norm_two, fc_weight) + fc_bias)))
    return (residual + low_back(matmul(hidden, proj_weight) + proj_bias)) * live_rows[:, None]

def reference(tokens, attn_gain, attn_shift, qkv_weight, qv_bias, out_weight, out_bias, mlp_gain, mlp_shift, fc_weight, fc_bias, proj_weight, proj_bias, out_grad, segment_ids):
    live_rows = (segment_ids < CAP).astype(jnp.float32)
    params_all = (tokens, attn_gain, attn_shift, qkv_weight, qv_bias, out_weight, out_bias, mlp_gain, mlp_shift, fc_weight, fc_bias, proj_weight, proj_bias)
    widened = [entry.astype(jnp.float32) for entry in params_all]
    result, pullback = jax.vjp(lambda *pieces: forward(*pieces, live_rows, segment_ids), *widened)
    grads = pullback(out_grad.astype(jnp.float32))
    return (result.astype(jnp.bfloat16), grads[0].astype(jnp.bfloat16), grads[1], grads[2], grads[3], grads[4], grads[5], grads[6], grads[7], grads[8], grads[9], grads[10], grads[11], grads[12])
```

```python
import math

import jax
import jax.numpy as jnp
from jax import lax
from jax.sharding import PartitionSpec as P

H = 25
HD = 64
BF = jnp.bfloat16
F32 = jnp.float32


def layer_norm(values, gain, shift):
    centre = values - jnp.mean(values, axis=-1, keepdims=True)
    spread = jnp.mean(centre * centre, axis=-1, keepdims=True)
    return centre * lax.rsqrt(spread + 1e-05) * gain + shift


def gelu_tanh(values):
    return jax.nn.gelu(values, approximate=True)


def times(left, right):
    return jnp.dot(left, right, preferred_element_type=F32)


def times_t(left, right):
    return lax.dot_general(left, right, (((1,), (1,)), ((), ())), preferred_element_type=F32)


def t_times(left, right):
    return lax.dot_general(left, right, (((0,), (0,)), ((), ())), preferred_element_type=F32)


def to_groups(array, per_group):
    capacity, head_count, head_size = array.shape
    return jnp.moveaxis(
        array.reshape(capacity, head_count // per_group, per_group, head_size), 1, 0
    )


def from_groups(array):
    groups, capacity, per_group, head_size = array.shape
    return jnp.moveaxis(array, 0, 1).reshape(capacity, groups * per_group * head_size)


def group_scores(query_part, key_part, allowed):
    head_size = query_part.shape[-1]
    scores = jnp.einsum(
        "qhd,khd->hqk", query_part, key_part, preferred_element_type=F32
    ) * head_size ** (-0.5)
    return jnp.where(allowed[None], scores, -1e30)


def attention_forward(queries, key_vecs, value_vecs, allowed, per_group):

    def group_forward(pieces):
        query_part, key_part, value_part = pieces
        scores = group_scores(query_part, key_part, allowed)
        row_max = jnp.max(scores, axis=-1, keepdims=True)
        logsum = row_max + jnp.log(jnp.sum(jnp.exp(scores - row_max), axis=-1, keepdims=True))
        prob_low = jnp.exp(scores - logsum).astype(BF)
        mixed_part = jnp.einsum("hqk,khd->qhd", prob_low, value_part, preferred_element_type=F32)
        return (mixed_part.astype(BF), logsum)

    mixed_parts, logsum = lax.map(
        group_forward,
        (
            to_groups(queries, per_group),
            to_groups(key_vecs, per_group),
            to_groups(value_vecs, per_group),
        ),
    )
    return (from_groups(mixed_parts), logsum)


def attention_backward(queries, key_vecs, value_vecs, logsum, mixed_grad, allowed, per_group):

    def group_backward(pieces):
        query_part, key_part, value_part, logsum_part, grad_part = pieces
        head_size = query_part.shape[-1]
        exact_probs = jnp.exp(group_scores(query_part, key_part, allowed) - logsum_part)
        probs_grad = jnp.einsum("qhd,khd->hqk", grad_part, value_part, preferred_element_type=F32)
        inner = jnp.sum(exact_probs * probs_grad, axis=-1, keepdims=True)
        scores_grad = (exact_probs * (probs_grad - inner)).astype(BF)
        query_grad = jnp.einsum(
            "hqk,khd->qhd", scores_grad, key_part, preferred_element_type=F32
        ) * head_size ** (-0.5)
        key_grad = jnp.einsum(
            "hqk,qhd->khd", scores_grad, query_part, preferred_element_type=F32
        ) * head_size ** (-0.5)
        value_grad = jnp.einsum(
            "hqk,qhd->khd", exact_probs.astype(BF), grad_part, preferred_element_type=F32
        )
        return (query_grad.astype(BF), key_grad.astype(BF), value_grad.astype(BF))

    query_grad, key_grad, value_grad = lax.map(
        group_backward,
        (
            to_groups(queries, per_group),
            to_groups(key_vecs, per_group),
            to_groups(value_vecs, per_group),
            logsum,
            to_groups(mixed_grad, per_group),
        ),
    )
    return jnp.concatenate(
        [from_groups(query_grad), from_groups(key_grad), from_groups(value_grad)], axis=1
    )


def layer_norm_back(centred, scale, grad, gain):
    n = centred * scale
    u = grad * gain
    part = scale * (
        u
        - jnp.mean(u, axis=-1, keepdims=True)
        - n * jnp.mean(u * n, axis=-1, keepdims=True)
    )
    return part, jnp.sum(grad * n, axis=0), jnp.sum(grad, axis=0)


def stats(values):
    centred = values - jnp.mean(values, axis=-1, keepdims=True)
    scale = lax.rsqrt(jnp.mean(centred * centred, axis=-1, keepdims=True) + 1e-05)
    return centred, scale


def make_block(reps, shards):
    chips = reps // 2

    def near(value, bits):
        return lax.ppermute(value, "shard", [(i, i ^ bits) for i in range(shards)])

    def other_core(value):
        return lax.ppermute(value, "rep", [(i, i ^ 1) for i in range(reps)])

    def chip_hop(value, pairs):
        return lax.ppermute(
            value,
            "rep",
            [(4 * 2 * g + 2 * a + c, 4 * 2 * g + 2 * b + c) for g in range(chips // 4) for a, b in pairs for c in range(2)],
        )

    def gather(value):
        if shards != 4:
            return [value] + [near(value, k) for k in range(1, shards)]
        cut = value.shape[0] // 16 * 8
        by_x, by_y = near(value, 1), near(value, 2)
        far = jnp.concatenate([near(by_y[:cut], 1), near(by_x[cut:], 2)], axis=0)
        return [value, by_x, by_y, far]

    def scatter_sum(parts):
        if shards != 4:
            total = parts[0].astype(F32)
            for k in range(1, shards):
                total = total + near(parts[k], k).astype(F32)
            return total
        own, for_x, for_y, far = parts
        cut = own.shape[0] // 16 * 8
        far_top, far_low = near(far[:cut], 1), near(far[cut:], 2)
        x_top, y_low = near(for_x[:cut], 1), near(for_y[cut:], 2)
        x_low = near((for_x[cut:].astype(F32) + far_low.astype(F32)).astype(BF), 1)
        y_top = near((for_y[:cut].astype(F32) + far_top.astype(F32)).astype(BF), 2)
        top = own[:cut].astype(F32) + x_top.astype(F32) + y_top.astype(F32)
        low = own[cut:].astype(F32) + x_low.astype(F32) + y_low.astype(F32)
        return jnp.concatenate([top, low], axis=0)

    def sum_over_chips(value):
        place = lax.axis_index("rep") // 2 % 4
        inner = (place == 1) | (place == 2)
        joined = (value.astype(F32) + chip_hop(value, [(0, 1), (3, 2)]).astype(F32)).astype(BF)
        total = (joined.astype(F32) + chip_hop(joined, [(1, 2), (2, 1)]).astype(F32)).astype(BF)
        step = 4
        while step < chips:
            other = lax.ppermute(total, "rep", [(i, i ^ (2 * step)) for i in range(reps)])
            total = (total.astype(F32) + other.astype(F32)).astype(BF)
            step *= 2
        back = chip_hop(total, [(1, 0), (2, 3)])
        return jnp.where(inner, total, back)

    def per_device(
        tokens,
        attn_gain,
        attn_shift,
        qkv_weight,
        qv_bias,
        out_weight,
        out_bias,
        mlp_gain,
        mlp_shift,
        fc_weight,
        fc_bias,
        proj_weight,
        proj_bias,
        out_grad,
        segment_ids,
    ):
        capacity, width = tokens.shape
        rows = qkv_weight.shape[0]
        half = rows // 2
        hidden_cols = proj_weight.shape[0]
        per_group = math.gcd(H, 5)
        core = lax.axis_index("rep") % 2
        member = lax.axis_index("shard")

        def place_rows(blocks, block_rows):
            full = jnp.zeros((shards * block_rows,) + blocks[0].shape[1:], blocks[0].dtype)
            for k, block in enumerate(blocks):
                at = ((member ^ k) * block_rows,) + (0,) * (block.ndim - 1)
                full = lax.dynamic_update_slice(full, block, at)
            return full

        def gather_weight(shard_rows):
            mine = lax.dynamic_slice_in_dim(shard_rows, core * half, half, axis=0)
            got = gather(mine)
            theirs = [None] + [other_core(block) for block in got[1:]]
            full = jnp.zeros((shards * rows,) + shard_rows.shape[1:], shard_rows.dtype)
            full = lax.dynamic_update_slice(full, shard_rows, (member * rows, 0))
            for k in range(1, shards):
                base = (member ^ k) * rows
                full = lax.dynamic_update_slice(full, got[k], (base + core * half, 0))
                full = lax.dynamic_update_slice(full, theirs[k], (base + (1 - core) * half, 0))
            return full

        smalls = (attn_gain, attn_shift, qv_bias, out_bias, mlp_gain, mlp_shift, proj_bias)
        packed = jnp.concatenate(smalls)[None]
        packed = [packed] + [near(packed, k) for k in range(1, shards)]
        packed = place_rows(packed, 1).astype(F32)
        wide = []
        at = 0
        for small in smalls:
            wide.append(packed[:, at : at + small.shape[0]].reshape(-1))
            at += small.shape[0]
        gain_one, shift_one, bias_qv, bias_out, gain_two, shift_two, bias_proj = wide

        full_qkv = gather_weight(qkv_weight)
        full_out = gather_weight(out_weight)

        live_rows = (segment_ids < capacity).astype(F32)[:, None]
        positions = jnp.arange(capacity)
        allowed = (segment_ids[:, None] == segment_ids[None, :]) & (
            positions[None, :] <= positions[:, None]
        )
        grad_out = out_grad.astype(F32) * live_rows
        grad_low = grad_out.astype(BF)
        grad_blocks = gather(grad_low)

        fc_cols = fc_weight.reshape(2, half, shards, hidden_cols)
        mine = lax.dynamic_index_in_dim(fc_cols, core, 0, keepdims=False)
        mine = jnp.moveaxis(mine, 1, 0)
        got = [lax.dynamic_index_in_dim(mine, member ^ k, 0, keepdims=False) for k in range(shards)]
        got = [got[0]] + [near(got[k], k) for k in range(1, shards)]
        theirs = [other_core(block) for block in got]
        fc_full = jnp.zeros((shards * rows, hidden_cols), BF)
        for k in range(shards):
            base = (member ^ k) * rows
            fc_full = lax.dynamic_update_slice(fc_full, got[k], (base + core * half, 0))
            fc_full = lax.dynamic_update_slice(fc_full, theirs[k], (base + (1 - core) * half, 0))

        inputs = tokens.astype(F32)
        norm_one = layer_norm(inputs, gain_one, shift_one).astype(BF)
        projected = times(norm_one, full_qkv)
        queries = (projected[:, 0:width] + bias_qv[0:width]).astype(BF)
        key_vecs = projected[:, width : 2 * width].astype(BF)
        value_vecs = (projected[:, 2 * width :] + bias_qv[width:]).astype(BF)
        queries = queries.reshape(capacity, H, HD)
        key_vecs = key_vecs.reshape(capacity, H, HD)
        value_vecs = value_vecs.reshape(capacity, H, HD)
        mixed_heads, logsum = attention_forward(queries, key_vecs, value_vecs, allowed, per_group)
        residual = inputs + times(mixed_heads, full_out) + bias_out
        norm_two = layer_norm(residual, gain_two, shift_two).astype(BF)

        norm_blocks = gather(norm_two)
        fc_bias_wide = fc_bias.astype(F32)
        hidden, pre_grad, out_parts, norm_parts = [], [], [], []
        for k in range(shards):
            pre_gelu = times(norm_blocks[k], fc_full) + fc_bias_wide
            act, back = jax.vjp(gelu_tanh, pre_gelu)
            hidden_grad = times_t(grad_blocks[k], proj_weight)
            hidden.append(act.astype(BF))
            pre_grad.append(back(hidden_grad)[0].astype(BF))
            out_parts.append(times(hidden[k], proj_weight).astype(BF))
            norm_parts.append(times_t(pre_grad[k], fc_full).astype(BF))
        norm_two_grad = scatter_sum(norm_parts)
        block_out = ((residual + scatter_sum(out_parts) + bias_proj) * live_rows).astype(BF)

        hidden_all = jnp.concatenate(hidden, axis=0)
        pre_all = jnp.concatenate(pre_grad, axis=0)
        grad_all = jnp.concatenate(grad_blocks, axis=0)
        norm_all = jnp.concatenate(norm_blocks, axis=0)
        proj_grad = t_times(hidden_all, grad_all).astype(BF).reshape(2, hidden_cols // 2, width)
        fc_grad = t_times(norm_all, pre_all).astype(BF).reshape(shards, 2, half, hidden_cols)
        fc_bias_grad = jnp.sum(pre_all, axis=0, dtype=F32)

        def core_sum(value, axis):
            keep = lax.dynamic_index_in_dim(value, core, axis, keepdims=False)
            give = lax.dynamic_index_in_dim(value, 1 - core, axis, keepdims=False)
            return (keep.astype(F32) + other_core(give).astype(F32)).astype(BF)

        def finish(mine_bf):
            theirs_bf = other_core(mine_bf)
            first = jnp.where(core == 0, mine_bf, theirs_bf)
            second = jnp.where(core == 0, theirs_bf, mine_bf)
            return first, second

        proj_mine = sum_over_chips(core_sum(proj_grad, 0))
        first, second = finish(proj_mine)
        proj_weight_grad = jnp.concatenate([first, second], axis=0).astype(F32)

        fc_mine = core_sum(fc_grad, 1)
        fc_blocks = [
            lax.dynamic_index_in_dim(fc_mine, member ^ k, 0, keepdims=False) for k in range(shards)
        ]
        fc_blocks = [fc_blocks[0]] + [near(fc_blocks[k], k) for k in range(1, shards)]
        fc_mine = place_rows([block[None] for block in fc_blocks], 1)
        fc_mine = sum_over_chips(fc_mine)
        first, second = finish(fc_mine)
        fc_weight_grad = jnp.moveaxis(jnp.concatenate([first, second], axis=1), 0, 1)
        fc_weight_grad = fc_weight_grad.reshape(rows, shards * hidden_cols).astype(F32)

        centred, scale = stats(residual)
        part, mlp_gain_grad, mlp_shift_grad = layer_norm_back(centred, scale, norm_two_grad, gain_two)
        residual_grad = grad_out + part
        residual_low = residual_grad.astype(BF)
        mixed_grad = times_t(residual_low, full_out).astype(BF).reshape(capacity, H, HD)

        def both_cores_half(value):
            cols = value.reshape(capacity, shards, 2, half)
            keep = lax.dynamic_index_in_dim(cols, core, 2, keepdims=False)
            give = lax.dynamic_index_in_dim(cols, 1 - core, 2, keepdims=False)
            both = jnp.concatenate([keep, other_core(give)], axis=0)
            return [
                lax.dynamic_index_in_dim(both, member ^ k, 1, keepdims=False) for k in range(shards)
            ]

        def both_cores(value):
            return jnp.concatenate([value, other_core(value)], axis=0)

        def weight_grad(left_blocks, right):
            parts = [t_times(left_blocks[k], right).astype(BF) for k in range(shards)]
            mine_bf = sum_over_chips(scatter_sum(parts).astype(BF))
            first, second = finish(mine_bf)
            return jnp.concatenate([first, second], axis=0).astype(F32)

        out_weight_grad = weight_grad(both_cores_half(mixed_heads), both_cores(residual_low))

        qkv_grad = attention_backward(
            queries, key_vecs, value_vecs, logsum, mixed_grad, allowed, per_group
        )
        qkv_weight_grad = weight_grad(both_cores_half(norm_one), both_cores(qkv_grad))
        norm_one_grad = times_t(qkv_grad, full_qkv)
        centred, scale = stats(inputs)
        part, attn_gain_grad, attn_shift_grad = layer_norm_back(centred, scale, norm_one_grad, gain_one)
        tokens_grad = (residual_grad + part).astype(BF)

        small_grads = (
            attn_gain_grad,
            attn_shift_grad,
            jnp.sum(qkv_grad[:, 0:width], axis=0, dtype=F32),
            jnp.sum(qkv_grad[:, 2 * width :], axis=0, dtype=F32),
            jnp.sum(residual_low, axis=0, dtype=F32),
            mlp_gain_grad,
            mlp_shift_grad,
            jnp.sum(grad_low, axis=0, dtype=F32),
        )
        vector = jnp.concatenate(small_grads)[None]
        step = 1
        while step < shards:
            vector = vector + near(vector, step)
            step *= 2
        vector = jnp.concatenate([vector, fc_bias_grad[None]], axis=1)
        step = 1
        while step < reps:
            vector = vector + lax.ppermute(vector, "rep", [(i, i ^ step) for i in range(reps)])
            step *= 2

        def own_slice(at, total):
            size = total // shards
            return lax.dynamic_slice(vector, (0, at + member * size), (1, size)).reshape(size)

        qv = lax.dynamic_slice(vector, (0, 2 * width + member * (2 * width // shards)), (1, 2 * width // shards))
        return (
            block_out,
            tokens_grad,
            own_slice(0, width),
            own_slice(width, width),
            qkv_weight_grad,
            qv.reshape(-1),
            out_weight_grad,
            own_slice(4 * width, width),
            own_slice(5 * width, width),
            own_slice(6 * width, width),
            fc_weight_grad,
            vector[0, 8 * width :],
            proj_weight_grad,
            own_slice(7 * width, width),
        )

    return per_device


def solution(mesh):
    per_device = make_block(mesh.shape["rep"], mesh.shape["shard"])
    rows = P(("rep", "shard"), None)
    flat, wide = P("shard"), P("shard", None)
    in_specs = (rows, flat, flat, wide, flat, wide, flat, flat, flat, wide, flat, wide, flat, rows, P(("rep", "shard")))
    out_specs = (rows, rows, flat, flat, wide, flat, wide, flat, flat, flat, wide, flat, wide, flat)
    return jax.shard_map(
        per_device, mesh=mesh, in_specs=in_specs, out_specs=out_specs, check_vma=False
    )
```
